32 devices in a mesh: sec: 8 (over y, x, core), pan: 4 (over z).
Axes of the slice: x: 2, y: 2, z: 4, core: 2. Of those that a mesh axis runs over, the one named last changes fastest.
Arguments:
- wave_state: bfloat16 [8, 512, 512], P('sec', 'pan'), may hold values from -6 to 6
- right_blocks: bfloat16 [8, 16, 512, 512], P('sec', None, None, 'pan'), may hold values from -0.25 to 0.25
- left_blocks: bfloat16 [576, 512, 512], P('sec', 'pan'), may hold values from -0.125 to 0.125
- coupling: bfloat16 [576], P('sec'), may hold values from -1 to 1
- channel_term: int32 [576], P('sec'), may hold values from 0 to 15
- channel_out: int32 [576], P('sec'), may hold values from 0 to 7, as said below
- sector_dims: int32 [8], P('sec'), may hold values from 128 to 512
Outputs:
- applied: float32 [8, 512, 512], P('sec', 'pan')
The draws below stay inside these ranges and needn't reach their ends.
Inputs may be any that keep to these rules, and one draw needn't show every extreme that they name: `channel_out`: channel c ends in a sector at most two away from the sector c // 72 that it starts from.
All inputs are finite; a program needn't handle non-finite values.
Results may differ from the reference program's by a relative error of at most 0.0041.
Values may be sent and summed in bfloat16 or wider, within the bound.
No kernel may reach another device: no remote copies, remote signals or barrier semaphores. Data moves between devices by JAX's collectives and lax.ppermute only.
A program may use at most 128 MiB of HBM per device.

```python
import jax
import jax.numpy as jnp
from jax import lax

DB = 512
NW = 16
CH_DEV = 72
SECTORS = 8
CHANNELS = 576


def draw_channel_out(key, part):
    chan_total = CH_DEV * SECTORS
    source = jnp.arange(chan_total, dtype=jnp.int32) // CH_DEV
    offset = jax.random.randint(key, (chan_total,), -2, 3, dtype=jnp.int32)
    return jnp.clip(source + offset, 0, SECTORS - 1).astype(jnp.int32)


def place_ends(drawn, stream_key, low, largest):
    longest = drawn.shape.index(max(drawn.shape))
    spots = []
    for shift in (0, 1):
        where = [jax.random.randint(jax.random.fold_in(stream_key, axis), (), 0, length) for axis, length in enumerate(drawn.shape)]
        where[longest] = (where[longest] + shift) % drawn.shape[longest]
        spots.append(tuple(where))
    return drawn.at[spots[0]].set(low).at[spots[1]].set(largest)


def block_scale(own_key, shape, pieces, smallest, largest):
    factor_of = 1.0
    for position, shards_of in pieces:
        draws = jax.random.uniform(jax.random.fold_in(jax.random.fold_in(own_key, 6), position), (shards_of,), jnp.float32, smallest / len(pieces), largest / len(pieces))
        factor_of = factor_of * jnp.repeat(jnp.exp(draws), shape[position] // shards_of).reshape((-1,) + (1,) * (len(shape) - 1 - position))
    return factor_of


def bell_draw(rng, extent, spread, reach, shards=(), kind=jnp.bfloat16):
    gain = block_scale(rng, extent, shards, -0.22, 0.18) if shards else 1.0
    drawn = jax.random.normal(rng, extent, jnp.float32) * spread * gain
    return jnp.minimum(jnp.maximum(drawn, -reach), reach).astype(kind)


def setup_inputs(seed: int = 0) -> dict:
    streams_of = jax.random.split(jax.random.key(seed), 8)
    return {
        "wave_state": bell_draw(streams_of[0], (SECTORS, DB, DB), 1.0, 6.0, ((0, 8), (1, 4))),
        "right_blocks": bell_draw(streams_of[1], (SECTORS, NW, DB, DB), DB ** -0.5, 0.25, ((0, 8), (3, 4))),
        "left_blocks": bell_draw(streams_of[2], (CHANNELS, DB, DB), (4 * DB) ** -0.5, 0.125, ((0, 8), (1, 4))),
        "coupling": jnp.clip(jax.random.uniform(streams_of[3], (CHANNELS,), jnp.float32, -1.0, 1.0) * block_scale(streams_of[3], (CHANNELS,), ((0, 8),), -0.4, 0.0), -1.0, 1.0).astype(jnp.bfloat16),
        "channel_term": place_ends(jax.random.randint(streams_of[4], (CHANNELS,), 0, NW), jax.random.fold_in(streams_of[4], 1), 0, NW - 1).astype(jnp.int32),
        "channel_out": draw_channel_out(jax.random.fold_in(streams_of[7], 71), 0),
        "sector_dims": place_ends(jax.random.randint(streams_of[6], (SECTORS,), DB // 4, DB + 1), jax.random.fold_in(streams_of[6], 1), DB // 4, DB).astype(jnp.int32),
    }


def reference(wave_state, right_blocks, left_blocks, coupling, channel_term, channel_out, sector_dims):
    indices = jnp.arange(DB, dtype=jnp.int32)
    slot_ids = jnp.arange(5, dtype=jnp.int32)
    term_ids = jnp.arange(NW, dtype=jnp.int32)

    def visit_sector(totals, sector):
        live_dim = sector_dims[sector]
        inside = (indices[:, None] < live_dim) & (indices[None, :] < live_dim)
        masked = jnp.where(inside, wave_state[sector], jnp.zeros((), jnp.bfloat16))
        terms_here = jnp.einsum("ik,wkq->wiq", masked.astype(jnp.float32), right_blocks[sector].astype(jnp.float32)).astype(jnp.bfloat16)
        first_chan = (sector * CH_DEV).astype(jnp.int32)
        left_part = lax.dynamic_slice_in_dim(left_blocks, first_chan, CH_DEV, 0)
        coef_part = lax.dynamic_slice_in_dim(coupling, first_chan, CH_DEV, 0)
        kind_part = lax.dynamic_slice_in_dim(channel_term, first_chan, CH_DEV, 0)
        targets = lax.dynamic_slice_in_dim(channel_out, first_chan, CH_DEV, 0)
        slot_index = targets - sector + 2
        chosen = (slot_index[None, None, :] == slot_ids[:, None, None]) & (kind_part[None, None, :] == term_ids[None, :, None])
        weights = jnp.where(chosen, coef_part[None, None, :], jnp.zeros((), jnp.bfloat16)).reshape(5 * NW, CH_DEV)
        combined = jnp.dot(weights, left_part.reshape(CH_DEV, DB * DB), preferred_element_type=jnp.float32)
        combined = combined.astype(jnp.bfloat16).reshape(5, NW, DB, DB)
        partial_value = jnp.einsum("jwri,wiq->jrq", combined.astype(jnp.float32), terms_here.astype(jnp.float32))
        window = lax.dynamic_slice_in_dim(totals, sector, 5, 0)
        totals = lax.dynamic_update_slice_in_dim(totals, window + partial_value, sector, 0)
        return totals, None

    start_totals = jnp.zeros((SECTORS + 4, DB, DB), jnp.float32)
    totals, _ = lax.scan(visit_sector, start_totals, jnp.arange(SECTORS, dtype=jnp.int32))
    summed = totals[2:SECTORS + 2]
    limits = sector_dims[:, None, None]
    kept_mask = (indices[None, :, None] < limits) & (indices[None, None, :] < limits)
    return jnp.where(kept_mask, summed, jnp.zeros((), jnp.float32))
```

```python
import jax
import jax.numpy as jnp
from jax import lax
from jax.sharding import PartitionSpec as P


def passed_along(value, axis, steps):
    count = lax.axis_size(axis)
    first, last = (max(0, -steps), min(count, count - steps))
    return lax.ppermute(value, axis, [(source, source + steps) for source in range(first, last)])


def gathered_rows(block, axis):
    count = lax.axis_size(axis)
    me = lax.axis_index(axis)
    rotated = [block]
    for shift in range(1, count):
        rotated.append(
            lax.ppermute(block, axis, [(s, (s + shift) % count) for s in range(count)])
        )
    ordered = rotated[::-1]
    twice = jnp.concatenate(ordered + ordered[:-1], axis=0)
    rows = block.shape[0]
    return lax.dynamic_slice_in_dim(twice, (count - 1 - me) * rows, count * rows, 0)


def on_device(
    wave_state, right_blocks, left_blocks, coupling, channel_term, channel_out, sector_dims
):
    panel_rows = wave_state.shape[1]
    block_width = wave_state.shape[2]
    term_count = right_blocks.shape[1]
    panel_cols = right_blocks.shape[3]
    channels = left_blocks.shape[0]
    sector = lax.axis_index("sec")
    count = lax.axis_size("pan")
    me = lax.axis_index("pan")
    live_dim = sector_dims[0]

    whole_state = gathered_rows(wave_state[0], "pan")

    pieces = 2
    per_piece = term_count // pieces
    own = [right_blocks[0, c * per_piece : (c + 1) * per_piece] for c in range(pieces)]
    from_left = {0: own}
    from_right = {0: own}
    for s in range(1, count):
        rightward = [(i, i + 1) for i in range(s - 1, count - 1)]
        leftward = [(i + 1, i) for i in range(0, count - s)]
        from_left[s] = [lax.ppermute(v, "pan", rightward) for v in from_left[s - 1]]
        from_right[s] = [lax.ppermute(v, "pan", leftward) for v in from_right[s - 1]]

    indices = lax.iota(jnp.int32, block_width)
    inside = (indices[:, None] < live_dim) & (indices[None, :] < live_dim)
    masked = jnp.where(inside, whole_state, jnp.zeros((), jnp.bfloat16))

    slot_ids = lax.iota(jnp.int32, 5)
    term_ids = lax.iota(jnp.int32, term_count)
    slot_index = channel_out - sector + 2
    chosen = (slot_index[None, None, :] == slot_ids[:, None, None]) & (
        channel_term[None, None, :] == term_ids[None, :, None]
    )
    weights = jnp.where(chosen, coupling[None, None, :], jnp.zeros((), jnp.bfloat16)).reshape(
        5 * term_count, channels
    )
    combined = jnp.dot(
        weights,
        left_blocks.reshape(channels, panel_rows * block_width),
        preferred_element_type=jnp.float32,
    )
    combined = combined.astype(jnp.bfloat16).reshape(5, term_count, panel_rows, block_width)

    def panel_result(chunks):
        total = None
        for c, chunk in enumerate(chunks):
            term = jnp.einsum(
                "ik,wkq->wiq", masked, chunk, preferred_element_type=jnp.float32
            ).astype(jnp.bfloat16)
            part = jnp.einsum(
                "jwri,wiq->jrq",
                combined[:, c * per_piece : (c + 1) * per_piece],
                term,
                preferred_element_type=jnp.float32,
            )
            total = part if total is None else total + part
        return total

    def exchanged(value):
        result = value[2]
        for offset in (-2, -1, 1, 2):
            sent = passed_along(value[offset + 2].astype(jnp.bfloat16), "sec", offset)
            result = result + sent.astype(jnp.float32)
        return result

    panels = {0: panel_result(own)}
    tail = {}
    for s in range(1, count):
        if 2 * s < count:
            panels[-s] = panel_result(from_left[s])
            panels[s] = panel_result(from_right[s])
        else:
            here = [
                jnp.where(me >= s, l, r) for l, r in zip(from_left[s], from_right[s])
            ]
            (tail if s == count - 1 else panels)[s] = panel_result(here)

    early = sorted(panels)
    early_sum = exchanged(jnp.concatenate([panels[k] for k in early], axis=2))
    placed = {
        k: early_sum[:, t * panel_cols : (t + 1) * panel_cols] for t, k in enumerate(early)
    }
    for k, value in tail.items():
        placed[k] = exchanged(value)
    strip = jnp.concatenate(
        [placed[k] if k in placed else placed[-k] for k in range(-(count - 1), count)], axis=1
    )
    collected = lax.dynamic_slice_in_dim(
        strip, (count - 1 - me) * panel_cols, count * panel_cols, 1
    )
    row_ids = me * panel_rows + lax.iota(jnp.int32, panel_rows)
    kept_mask = (row_ids[:, None] < live_dim) & (indices[None, :] < live_dim)
    return jnp.where(kept_mask, collected, jnp.zeros((), jnp.float32))[None]


def solution(mesh):
    return jax.shard_map(
        on_device,
        mesh=mesh,
        in_specs=(
            P("sec", "pan", None),
            P("sec", None, None, "pan"),
            P("sec", "pan", None),
            P("sec"),
            P("sec"),
            P("sec"),
            P("sec"),
        ),
        out_specs=P("sec", "pan", None),
        check_vma=False,
    )
```

```python
import jax
import jax.numpy as jnp
from jax import lax
from jax.experimental import pallas as pl
from jax.experimental.pallas import tpu as pltpu
from jax.sharding import PartitionSpec as P


def passed_along(value, axis, steps):
    count = lax.axis_size(axis)
    first, last = (max(0, -steps), min(count, count - steps))
    return lax.ppermute(value, axis, [(source, source + steps) for source in range(first, last)])


def gathered_rows(block, axis):
    count = lax.axis_size(axis)
    me = lax.axis_index(axis)
    rotated = [block]
    for shift in range(1, count):
        rotated.append(
            lax.ppermute(block, axis, [(s, (s + shift) % count) for s in range(count)])
        )
    ordered = rotated[::-1]
    twice = jnp.concatenate(ordered + ordered[:-1], axis=0)
    rows = block.shape[0]
    return lax.dynamic_slice_in_dim(twice, (count - 1 - me) * rows, count * rows, 0)


def combine_kernel(place_ref, coef_ref, left_ref, out_ref, sums_ref):
    sums_ref[...] = jnp.zeros(sums_ref.shape, jnp.float32)

    def add_channel(c, carry):
        spot = place_ref[c]
        sums_ref[spot] += coef_ref[c] * left_ref[c].astype(jnp.float32)
        return carry

    lax.fori_loop(0, left_ref.shape[0], add_channel, 0)
    out_ref[...] = sums_ref[...].astype(jnp.bfloat16)


def combined_blocks(left_blocks, coupling, place, spots):
    channels, rows, width = left_blocks.shape
    step = min(rows, 32)
    return pl.pallas_call(
        combine_kernel,
        grid=(rows // step,),
        in_specs=[
            pl.BlockSpec(memory_space=pltpu.SMEM),
            pl.BlockSpec(memory_space=pltpu.SMEM),
            pl.BlockSpec((channels, step, width), lambda r: (0, r, 0)),
        ],
        out_specs=pl.BlockSpec((spots, step, width), lambda r: (0, r, 0)),
        out_shape=jax.ShapeDtypeStruct((spots, rows, width), jnp.bfloat16),
        scratch_shapes=[pltpu.VMEM((spots, step, width), jnp.float32)],
        name="combine",
    )(place, coupling.astype(jnp.float32), left_blocks)


def on_device(
    wave_state, right_blocks, left_blocks, coupling, channel_term, channel_out, sector_dims
):
    panel_rows = wave_state.shape[1]
    block_width = wave_state.shape[2]
    term_count = right_blocks.shape[1]
    panel_cols = right_blocks.shape[3]
    sector = lax.axis_index("sec")
    count = lax.axis_size("pan")
    me = lax.axis_index("pan")
    live_dim = sector_dims[0]

    whole_state = gathered_rows(wave_state[0], "pan")

    lent = term_count // 4 if count >= 4 else 0
    middle = (lent + term_count) // 2
    bounds = [(lent, middle), (middle, term_count)] + ([(0, lent)] if lent else [])
    own = [right_blocks[0, low:high] for low, high in bounds]
    from_left = {0: own}
    from_right = {0: own}
    for s in range(1, count):
        from_left[s] = []
        from_right[s] = []
        for k, (low, _) in enumerate(bounds):
            short = 1 if lent and low == 0 else 0
            rightward = [(i, i + 1) for i in range(s - 1, count - 1 - short)]
            leftward = [(i + 1, i) for i in range(short, count - s)]
            if rightward:
                from_left[s].append(lax.ppermute(from_left[s - 1][k], "pan", rightward))
                from_right[s].append(lax.ppermute(from_right[s - 1][k], "pan", leftward))

    slot_index = channel_out - sector + 2
    combined = combined_blocks(
        left_blocks, coupling, channel_term * 5 + slot_index, 5 * term_count
    ).reshape(term_count, 5, panel_rows, block_width)
    if lent:
        lent_rows = lax.ppermute(combined[:lent], "pan", [(0, 1), (count - 1, count - 2)])

    indices = lax.iota(jnp.int32, block_width)
    inside = (indices[:, None] < live_dim) & (indices[None, :] < live_dim)
    masked = jnp.where(inside, whole_state, jnp.zeros((), jnp.bfloat16))

    def term_of(chunk):
        return jnp.einsum(
            "ik,wkq->wiq", masked, chunk, preferred_element_type=jnp.float32
        ).astype(jnp.bfloat16)

    def contracted(rows, term):
        return jnp.einsum("wjri,wiq->jrq", rows, term, preferred_element_type=jnp.float32)

    def panel_result(terms):
        total = None
        for (low, high), term in zip(bounds, terms):
            part = contracted(combined[low:high], term)
            total = part if total is None else total + part
        return total

    def exchanged(value):
        result = value[2]
        for offset in (-2, -1, 1, 2):
            sent = passed_along(value[offset + 2].astype(jnp.bfloat16), "sec", offset)
            result = result + sent.astype(jnp.float32)
        return result

    terms = [term_of(v) for v in own]
    panels = {0: panel_result(terms)}
    lent_parts = [contracted(lent_rows, terms[-1])] if lent else []
    tail = {}
    for s in range(1, count):
        if 2 * s < count:
            left_terms = [term_of(v) for v in from_left[s]]
            right_terms = [term_of(v) for v in from_right[s]]
            panels[-s] = panel_result(left_terms)
            panels[s] = panel_result(right_terms)
            if lent:
                shared = jnp.where(me == 1, right_terms[-1], left_terms[-1])
        else:
            here = [
                term_of(jnp.where(me >= s, l, r)) for l, r in zip(from_left[s], from_right[s])
            ]
            (tail if s == count - 1 else panels)[s] = panel_result(here)
            shared = here[-1]
        if lent and s < count - 1:
            lent_parts.append(contracted(lent_rows, shared))

    early = sorted(panels)
    early_sum = exchanged(jnp.concatenate([panels[k] for k in early], axis=2))
    placed = {
        k: early_sum[:, t * panel_cols : (t + 1) * panel_cols] for t, k in enumerate(early)
    }
    returned = {}
    if lent:
        done = exchanged(jnp.concatenate(lent_parts, axis=2)).astype(jnp.bfloat16)
        back = lax.ppermute(done, "pan", [(1, 0), (count - 2, count - 1)])
        for s in range(count - 1):
            returned[s + 1] = back[:, s * panel_cols : (s + 1) * panel_cols].astype(jnp.float32)
    for k, value in tail.items():
        placed[k] = exchanged(value)

    def strip_at(k):
        value = placed[k] if k in placed else placed[-k]
        return value + returned[abs(k)] if abs(k) in returned else value

    strip = jnp.concatenate([strip_at(k) for k in range(-(count - 1), count)], axis=1)
    collected = lax.dynamic_slice_in_dim(
        strip, (count - 1 - me) * panel_cols, count * panel_cols, 1
    )
    row_ids = me * panel_rows + lax.iota(jnp.int32, panel_rows)
    kept_mask = (row_ids[:, None] < live_dim) & (indices[None, :] < live_dim)
    return jnp.where(kept_mask, collected, jnp.zeros((), jnp.float32))[None]


def solution(mesh):
    return jax.shard_map(
        on_device,
        mesh=mesh,
        in_specs=(
            P("sec", "pan", None),
            P("sec", None, None, "pan"),
            P("sec", "pan", None),
            P("sec"),
            P("sec"),
            P("sec"),
            P("sec"),
        ),
        out_specs=P("sec", "pan", None),
        check_vma=False,
    )
```
